16 devices in a mesh: dp: 2 (over z), sp: 8 (over y, x, core).
Axes of the slice: x: 2, y: 2, z: 2, core: 2. Of those that a mesh axis runs over, the one named last changes fastest.
Arguments:
- x: bfloat16 [16, 2048], P('dp'), parts along dimension 0
- lens: int32 [16], P('dp'), parts along dimension 0
- wq: bfloat16 [2, 2048, 2048], replicated
- wk: bfloat16 [2, 2048, 512], replicated
- wv: bfloat16 [2, 2048, 512], replicated
- wo: bfloat16 [2, 2048, 2048], P(None, 'sp')
- w1: bfloat16 [2, 2048, 8192], P(None, None, 'sp')
- w2: bfloat16 [2, 8192, 2048], P(None, 'sp')
- g1: bfloat16 [2, 2048], replicated
- g2: bfloat16 [2, 2048], replicated
- kc: bfloat16 [2, 16, 4096, 8, 64], P(None, 'dp', 'sp'), parts along dimension 1
- vc: bfloat16 [2, 16, 4096, 8, 64], P(None, 'dp', 'sp'), parts along dimension 1
Outputs:
- output 1: bfloat16 [16, 2048], P('dp'), parts along dimension 0
- output 2: bfloat16 [2, 16, 4096, 8, 64], P(None, 'dp', 'sp'), parts along dimension 1
- output 3: bfloat16 [2, 16, 4096, 8, 64], P(None, 'dp', 'sp'), parts along dimension 1
There are 2 independent parts. The reference program is written for one: setup_inputs(seed, part) draws one part's arguments, and reference() takes and returns one part's arrays. A program takes and returns all parts, laid end to end along the dimension named above; an argument that names none is the same for every part.
All inputs are finite; a program needn't handle non-finite values.
Results may differ from the reference program's by a relative error of at most 0.00905547.
Values are sent between devices in bfloat16 or wider.
A program may use at most 1 GiB of HBM per device.

```python
import math
import jax
import jax.numpy as jnp
from jax import lax

B = 8
S_DEV = 512
SEQ = 8
D = 2048
HEADS = 32
KV_HEADS = 8
HEAD = 64
LAYERS = 2
S = S_DEV * SEQ
G = HEADS // KV_HEADS
FF = 4 * D
BLOCK = min(S_DEV, 1024)
EPS = 1e-6


def _rms(h, g):
    r = lax.rsqrt(jnp.mean(h * h, axis=-1, keepdims=True) + EPS)
    return (h * r * g.astype(jnp.float32)).astype(jnp.bfloat16)


def _mm(a, w):
    return jnp.dot(a, w, preferred_element_type=jnp.float32)


def _cache(key, t):
    k = jax.random.split(key, 7)
    ph = jax.random.uniform(k[0], (B, 3), jnp.float32)
    fr = jax.random.uniform(k[1], (B, 3), jnp.float32, 1.0, 3.0)
    wave = jnp.sin(2.0 * math.pi * (fr[:, None, :] * t[None, :, None] + ph[:, None, :]))
    kdir = jax.random.normal(k[2], (B, 1, KV_HEADS, HEAD), jnp.float32)
    u1 = jax.random.normal(k[3], (B, 1, KV_HEADS, HEAD), jnp.float32)
    u2 = jax.random.normal(k[4], (B, 1, KV_HEADS, HEAD), jnp.float32)
    kc = jax.random.normal(k[5], (B, S, KV_HEADS, HEAD), jnp.float32) + wave[:, :, 0, None, None] * kdir
    vc = (0.5 * jax.random.normal(k[6], (B, S, KV_HEADS, HEAD), jnp.float32)
          + wave[:, :, 1, None, None] * u1 + wave[:, :, 2, None, None] * u2)
    return kc.astype(jnp.bfloat16), vc.astype(jnp.bfloat16)


def _lengths(key):
    draws = jax.random.randint(key, (B,), 0, 256, dtype=jnp.int32)
    scaled = draws * (S - 1) // 255
    lens = scaled * draws // 255 + 1
    return lens.at[0].set(S).astype(jnp.int32)


def setup_inputs(seed: int = 0, part: int = 0) -> dict:
    key = jax.random.key(seed)
    ks = jax.random.split(key, 8)
    kp = jax.random.split(jax.random.fold_in(key, part), 3)
    gamma = (math.log(S) - 1.0) / math.sqrt(HEAD)
    wk = jax.random.normal(ks[0], (LAYERS, D, KV_HEADS, 1, HEAD), jnp.float32) * D ** -0.5
    wq = gamma * wk + jax.random.normal(ks[1], (LAYERS, D, KV_HEADS, G, HEAD), jnp.float32) * D ** -0.5
    wv = jax.random.normal(ks[2], (LAYERS, D, KV_HEADS * HEAD), jnp.float32) * D ** -0.5
    wo = jax.random.normal(ks[3], (LAYERS, HEADS * HEAD, D), jnp.float32) * (HEADS * HEAD) ** -0.5
    w1 = jax.random.normal(ks[4], (LAYERS, D, FF), jnp.float32) * D ** -0.5
    w2 = jax.random.normal(ks[5], (LAYERS, FF, D), jnp.float32) * FF ** -0.5
    g1 = 1.0 + 0.1 * jax.random.normal(ks[6], (LAYERS, D), jnp.float32)
    g2 = 1.0 + 0.1 * jax.random.normal(ks[7], (LAYERS, D), jnp.float32)
    t = jnp.arange(S, dtype=jnp.float32) / S
    ck = jax.random.split(kp[2], LAYERS)
    caches = [_cache(ck[i], t) for i in range(LAYERS)]
    bf = jnp.bfloat16
    return {
        'x': jax.random.normal(kp[0], (B, D), jnp.float32).astype(bf),
        'lens': _lengths(kp[1]),
        'wq': wq.reshape(LAYERS, D, HEADS * HEAD).astype(bf),
        'wk': wk.reshape(LAYERS, D, KV_HEADS * HEAD).astype(bf),
        'wv': wv.astype(bf),
        'wo': wo.astype(bf),
        'w1': w1.astype(bf),
        'w2': w2.astype(bf),
        'g1': g1.astype(bf),
        'g2': g2.astype(bf),
        'kc': jnp.stack([c[0] for c in caches]),
        'vc': jnp.stack([c[1] for c in caches]),
    }


def _attend(q, kc, vc, lens):
    qf = q.astype(jnp.float32)

    def body(carry, i):
        m, l, o = carry
        k = lax.dynamic_slice_in_dim(kc, i * BLOCK, BLOCK, axis=1).astype(jnp.float32)
        v = lax.dynamic_slice_in_dim(vc, i * BLOCK, BLOCK, axis=1).astype(jnp.float32)
        s = jnp.einsum('bkgd,bskd->bkgs', qf, k) * HEAD ** -0.5
        posn = i * BLOCK + jnp.arange(BLOCK)
        s = jnp.where((posn[None, :] < lens[:, None])[:, None, None, :], s, -jnp.inf)
        mn = jnp.maximum(m, jnp.max(s, axis=-1))
        c = jnp.exp(m - mn)
        p = jnp.exp(s - mn[..., None])
        o = o * c[..., None] + jnp.einsum('bkgs,bskd->bkgd', p, v)
        return (mn, l * c + jnp.sum(p, axis=-1), o), None

    init = (jnp.full((B, KV_HEADS, G), -jnp.inf, jnp.float32),
            jnp.zeros((B, KV_HEADS, G), jnp.float32),
            jnp.zeros((B, KV_HEADS, G, HEAD), jnp.float32))
    (m, l, o), _ = lax.scan(body, init, jnp.arange(S // BLOCK))
    return o / l[..., None]


def reference(x, lens, wq, wk, wv, wo, w1, w2, g1, g2, kc, vc):
    posn = jnp.arange(S)
    write = (posn[None, :] == (lens - 1)[:, None])[:, :, None, None]

    def layer(h, w):
        wq_, wk_, wv_, wo_, w1_, w2_, g1_, g2_, kc_, vc_ = w
        xn = _rms(h, g1_)
        q = _mm(xn, wq_).astype(jnp.bfloat16).reshape(B, KV_HEADS, G, HEAD)
        k = _mm(xn, wk_).astype(jnp.bfloat16).reshape(B, 1, KV_HEADS, HEAD)
        v = _mm(xn, wv_).astype(jnp.bfloat16).reshape(B, 1, KV_HEADS, HEAD)
        kn = jnp.where(write, k, kc_)
        vn = jnp.where(write, v, vc_)
        o = _attend(q, kn, vn, lens).astype(jnp.bfloat16).reshape(B, HEADS * HEAD)
        h = h + _mm(o, wo_)
        u = jax.nn.gelu(_mm(_rms(h, g2_), w1_)).astype(jnp.bfloat16)
        h = h + _mm(u, w2_)
        return h, (kn, vn)

    h, (kn, vn) = lax.scan(layer, x.astype(jnp.float32), (wq, wk, wv, wo, w1, w2, g1, g2, kc, vc))
    return h.astype(jnp.bfloat16), kn, vn
```

```python
import functools
import math

import jax
import jax.numpy as jnp
from jax import lax
from jax.experimental import pallas as pl
from jax.experimental.pallas import tpu as pltpu
from jax.sharding import PartitionSpec as P

EPS = 1e-6
F32 = jnp.float32
BF16 = jnp.bfloat16
MESH = pl.DeviceIdType.MESH
HBM = pl.BlockSpec(memory_space=pl.ANY)
VMEM = pl.BlockSpec(memory_space=pltpu.VMEM)
SMEM = pl.BlockSpec(memory_space=pltpu.SMEM)
N = 8
CH = 256


def _rms(h, g):
    r = lax.rsqrt(jnp.mean(h * h, axis=-1, keepdims=True) + EPS)
    return (h * r * g.astype(F32)).astype(BF16)


def _iota(shape, dim):
    return lax.broadcasted_iota(jnp.int32, shape, dim)


def _attend(l, first, *refs):
    h_ref, lens, g1, wq, wk, wv, kc, vc = refs[:8]
    refs = refs[8:] if first else refs[10:]
    out, ko, vo, w, kb, vb, qs, ps, st, wsem, ksem, vsem, kosem, vosem = refs
    b, s = kb.shape[0], kb.shape[2]

    loads = [pltpu.make_async_copy(wk.at[l], w.at[0], wsem.at[0]),
             pltpu.make_async_copy(wv.at[l], w.at[1], wsem.at[1])]
    for i in range(4):
        loads.append(pltpu.make_async_copy(wq.at[l, :, pl.ds(512 * i, 512)], w.at[2 + i], wsem.at[2 + i]))
    kin = [pltpu.make_async_copy(kc.at[l, i], kb.at[i], ksem.at[i]) for i in range(b)]
    vin = [pltpu.make_async_copy(vc.at[l, i], vb.at[i], vsem.at[i]) for i in range(b)]
    kout = [pltpu.make_async_copy(kb.at[i], ko.at[l, i], kosem.at[i]) for i in range(b)]
    vout = [pltpu.make_async_copy(vb.at[i], vo.at[l, i], vosem.at[i]) for i in range(b)]
    for c in loads + kin + vin:
        c.start()

    xn = _rms(h_ref[...].astype(F32), g1[l:l + 1, :])
    proj = []
    for i in range(6):
        loads[i].wait()
        proj.append(jnp.dot(xn, w[i], preferred_element_type=F32).astype(BF16).astype(F32))
    knew, vnew = proj[0], proj[1]

    lane = _iota((8, 128), 1)
    for r in range(32):
        t = proj[2 + r // 8][:, (r // 2 % 4) * 128:(r // 2 % 4) * 128 + 128]
        half = r // 4 % 2
        if r % 2 != half:
            t = pltpu.roll(t, 64, 1)
        qs[r * 8:r * 8 + 8, :] = jnp.where(lane // 64 == half, t, 0.0)

    base = lax.axis_index('sp') * s

    def write(buf, new, i):
        pos = lens[i] - 1 - base

        @pl.when((pos >= 0) & (pos < s))
        def _():
            blk = pl.multiple_of(pos // 128 * 128, 128)
            col = jnp.broadcast_to(new[i:i + 1, :], (128, s)).T
            hit = _iota((s, 128), 1) == pos % 128
            old = buf[i, :, pl.ds(blk, 128)].astype(F32)
            buf[i, :, pl.ds(blk, 128)] = jnp.where(hit, col, old).astype(BF16)

    for i in range(b):
        kin[i].wait()
        write(kb, knew, i)
        kout[i].start()
    slane = _iota((32, 128), 1)
    for i in range(b):
        sc = []
        for kp in range(4):
            q = qs[pl.ds(kp * 64 + i, 8, stride=8), :].astype(BF16)
            sc.append(jnp.dot(q, kb[i, kp * 128:kp * 128 + 128, :], preferred_element_type=F32))
        sc = jnp.concatenate(sc, axis=0) * 0.125
        sc = jnp.where(_iota((32, s), 1) < lens[i] - base, sc, -jnp.inf)
        m = jnp.max(sc, axis=1, keepdims=True)
        p = jnp.exp(sc - jnp.where(m == -jnp.inf, 0.0, m))
        den = jnp.sum(p, axis=1, keepdims=True)
        ps[i] = p.astype(BF16)
        st[i] = jnp.where(slane % 64 < 32, m, den)

    for i in range(b):
        vin[i].wait()
        write(vb, vnew, i)
        vout[i].start()
    mine = _iota((8, 128), 0) // 4 == lane // 64
    for i in range(b):
        for grp in range(2):
            o = lax.dot_general(ps[i, grp * 16:grp * 16 + 16, :], vb[i, grp * 256:grp * 256 + 256, :],
                                (((1,), (1,)), ((), ())), preferred_element_type=F32)
            for half in range(2):
                kp = grp * 2 + half
                v = jnp.where(mine, o[half * 8:half * 8 + 8, half * 128:half * 128 + 128],
                              st[i, kp * 8:kp * 8 + 8, :])
                out[pl.ds(kp * 64 + i, 4, stride=8), :] = v[0:4]
                out[pl.ds(kp * 64 + 32 + i, 4, stride=8), :] = v[4:8]
    for c in kout + vout:
        c.wait()


def _finish(l, h_ref, att, g2, wo, w1, w2, out, wob, w1b, w2b, arecv, psend, rrecv, hb, xn,
            wsem, asem, asem2, rsem, rsem2, gsem, gsem2):
    me = lax.axis_index('sp')
    loads = [pltpu.make_async_copy(src.at[l], dst, wsem.at[i])
             for i, (src, dst) in enumerate(((wo, wob), (w1, w1b), (w2, w2b)))]
    barrier = pltpu.get_barrier_semaphore()
    peer = [lax.rem(me + i, N) for i in range(N)]
    for i in range(1, N):
        pl.semaphore_signal(barrier, inc=1, device_id={'sp': peer[i]}, device_id_type=MESH)
    for c in loads:
        c.start()
    pl.semaphore_wait(barrier, N - 1)

    sent = []

    def send(src, dst, s0, s1, i):
        c = pltpu.make_async_remote_copy(src, dst, s0, s1, device_id={'sp': peer[i]}, device_id_type=MESH)
        c.start()
        sent.append(c)
        return c

    parts = [send(att.at[pl.ds(pl.multiple_of(peer[i] * 32, 32), 32), :], arecv.at[i - 1],
                  asem.at[i - 1], asem2.at[i - 1], i) for i in range(1, N)]
    tiles = [att[pl.ds(pl.multiple_of(me * 32, 32), 32), :]]
    for i in range(1, N):
        parts[i - 1].wait_recv()
        tiles.append(arecv[i - 1])
    lane = _iota((32, 128), 1)
    low = lane % 64 < 32
    ms, ls = [], []
    for t in tiles:
        r = pltpu.roll(t, 64, 1)
        ms.append(jnp.where(low, r, pltpu.roll(r, 32, 1)))
        ls.append(jnp.where(low, pltpu.roll(r, 96, 1), r))
    top = functools.reduce(jnp.maximum, ms)
    num, den = jnp.zeros_like(top), jnp.zeros_like(top)
    for t, m, d in zip(tiles, ms, ls):
        c = jnp.exp(m - top)
        num, den = num + c * t, den + c * d
    o = num / den
    even = jnp.broadcast_to(lax.rem(me, 2) == 0, o.shape)
    o = jnp.where(even, o, pltpu.roll(o, 64, 1))
    other = pltpu.roll(o, 64, 1)
    first = _iota((8, 128), 1) < 64
    lhs = jnp.concatenate([jnp.where(first, o[t * 16:t * 16 + 8], other[t * 16 + 8:t * 16 + 16])
                           for t in range(2)], axis=1).astype(BF16)

    def summed(k, lhs, w, resid):
        hops = []
        for i in range(1, N):
            cols = pl.ds(pl.multiple_of(peer[i] * CH, CH), CH)
            psend[k, i - 1] = jnp.dot(lhs, w[:, cols], preferred_element_type=F32)
            hops.append(send(psend.at[k, i - 1], rrecv.at[k, i - 1], rsem.at[k, i - 1], rsem2.at[k, i - 1], i))
        cols = pl.ds(pl.multiple_of(me * CH, CH), CH)
        acc = jnp.dot(lhs, w[:, cols], preferred_element_type=F32)
        for i in range(1, N):
            hops[i - 1].wait_recv()
            acc = acc + rrecv[k, i - 1]
        hb[k, me] = resid() + acc
        hops = [send(hb.at[k, me], hb.at[k, me], gsem.at[k, i - 1], gsem2.at[k, i - 1], i) for i in range(1, N)]
        for c in hops:
            c.wait_recv()

    loads[0].wait()
    summed(0, lhs, wob, lambda: h_ref[:, pl.ds(pl.multiple_of(me * CH, CH), CH)].astype(F32))
    hs = [hb[0, c] for c in range(N)]
    ss = sum(jnp.sum(x * x, axis=1, keepdims=True) for x in hs)
    r = lax.rsqrt(ss / (N * CH) + EPS)
    for c in range(N):
        g = g2[l:l + 1, c * CH:(c + 1) * CH].astype(F32)
        xn[:, c * CH:(c + 1) * CH] = (hs[c] * r * g).astype(BF16)
    loads[1].wait()
    u = jax.nn.gelu(jnp.dot(xn[...], w1b[...], preferred_element_type=F32)).astype(BF16)
    loads[2].wait()
    summed(1, u, w2b, lambda: hb[0, me])
    for c in range(N):
        out[:, c * CH:(c + 1) * CH] = hb[1, c].astype(out.dtype)
    for c in sent:
        c.wait_send()


def solution(mesh):
    kspec = P(None, 'dp', 'sp', None, None)
    DMA = pltpu.SemaphoreType.DMA

    def attend(l, h, lens, g1, wq, wk, wv, kt, vt, bufs):
        nl, b, d, s = kt.shape
        cache = jax.ShapeDtypeStruct(kt.shape, kt.dtype)
        first = not bufs
        return pl.pallas_call(
            functools.partial(_attend, l, first),
            out_shape=(jax.ShapeDtypeStruct((256, 128), F32), cache, cache),
            in_specs=[VMEM, SMEM, VMEM] + [HBM] * (5 if first else 7),
            out_specs=(VMEM, HBM, HBM),
            input_output_aliases={} if first else {8: 1, 9: 2},
            scratch_shapes=[
                pltpu.VMEM((6, wq.shape[1], 512), BF16),
                pltpu.VMEM((b, d, s), BF16), pltpu.VMEM((b, d, s), BF16),
                pltpu.VMEM((256, 128), F32), pltpu.VMEM((b, 32, s), BF16), pltpu.VMEM((b, 32, 128), F32),
                DMA((6,)), DMA((b,)), DMA((b,)), DMA((b,)), DMA((b,))],
            compiler_params=pltpu.CompilerParams(vmem_limit_bytes=60 << 20),
            name=f'attend{l}',
        )(h, lens, g1, wq, wk, wv, kt, vt, *bufs)

    def finish(l, h, att, g2, wo, w1, w2, dtype):
        return pl.pallas_call(
            functools.partial(_finish, l),
            out_shape=jax.ShapeDtypeStruct(h.shape, dtype),
            in_specs=[VMEM, VMEM, VMEM, HBM, HBM, HBM],
            out_specs=VMEM,
            scratch_shapes=[
                pltpu.VMEM(wo.shape[1:], BF16), pltpu.VMEM(w1.shape[1:], BF16), pltpu.VMEM(w2.shape[1:], BF16),
                pltpu.VMEM((N - 1, 32, 128), F32),
                pltpu.VMEM((2, N - 1, 8, CH), F32), pltpu.VMEM((2, N - 1, 8, CH), F32),
                pltpu.VMEM((2, N, 8, CH), F32), pltpu.VMEM(h.shape, BF16),
                DMA((3,)), DMA((N - 1,)), DMA((N - 1,)),
                DMA((2, N - 1)), DMA((2, N - 1)), DMA((2, N - 1)), DMA((2, N - 1))],
            compiler_params=pltpu.CompilerParams(collective_id=l, has_side_effects=True, vmem_limit_bytes=60 << 20),
            name=f'finish{l}',
        )(h, att, g2, wo, w1, w2)

    def local(x, lens, wq, wk, wv, wo, w1, w2, g1, g2, kc, vc):
        nl, b, s, kvh, dh = kc.shape
        kt = kc.transpose(0, 1, 3, 4, 2).reshape(nl, b, kvh * dh, s)
        vt = vc.transpose(0, 1, 3, 4, 2).reshape(nl, b, kvh * dh, s)
        h, bufs = x, ()
        for l in range(nl):
            att, *bufs = attend(l, h, lens, g1, wq, wk, wv, kt, vt, bufs)
            h = finish(l, h, att, g2, wo, w1, w2, BF16 if l == nl - 1 else F32)
        back = [t.reshape(nl, b, kvh, dh, s).transpose(0, 1, 4, 2, 3) for t in bufs]
        return h, *back

    return jax.shard_map(
        local, mesh=mesh,
        in_specs=(P('dp', None), P('dp'), P(), P(), P(), P(None, 'sp', None), P(None, None, 'sp'),
                  P(None, 'sp', None), P(), P(), kspec, kspec),
        out_specs=(P('dp', None), kspec, kspec), check_vma=False)
```

```python
import functools

import jax
import jax.numpy as jnp
from jax import lax
from jax.experimental import pallas as pl
from jax.experimental.pallas import tpu as pltpu
from jax.sharding import PartitionSpec as P

EPS = 1e-6
F32 = jnp.float32
BF16 = jnp.bfloat16
MESH = pl.DeviceIdType.MESH
HBM = pl.BlockSpec(memory_space=pl.ANY)
VMEM = pl.BlockSpec(memory_space=pltpu.VMEM)
SMEM = pl.BlockSpec(memory_space=pltpu.SMEM)
DMA = pltpu.SemaphoreType.DMA
N = 8
HALF = 1024


def _in(space, *arrays):
    return [pltpu.with_memory_space_constraint(a, space) for a in arrays]


def _iota(shape, dim):
    return lax.broadcasted_iota(jnp.int32, shape, dim)


def _peer(me, k):
    y, x, c = me // 4, me // 2 % 2, me % 2
    return (y + k // 4) % 2 * 4 + (x + k // 2 % 2) % 2 * 2 + (c + k % 2) % 2


def _project(h, g, w, wait):
    r = lax.rsqrt(jnp.mean(h * h, axis=-1, keepdims=True) + EPS)
    xn = (h * r * g).astype(BF16)
    out = []
    for i in range(6):
        wait(i)
        out.append(jnp.dot(xn, w[i], preferred_element_type=F32).astype(BF16).astype(F32))
    return out


def _partials(proj, lens, base, kb, vb, kwait, vwait, qs, sn, ps, pn, st, out):
    knew, vnew = proj[0], proj[1]
    b, s = kb.shape[0], kb.shape[2]
    lane = _iota((8, 128), 1)
    for r in range(32):
        t = proj[2 + r // 8][:, (r // 2 % 4) * 128:(r // 2 % 4) * 128 + 128]
        half = r // 4 % 2
        if r % 2 != half:
            t = pltpu.roll(t, 64, 1)
        t = jnp.where(lane // 64 == half, t, 0.0)
        qs[r * 8:r * 8 + 8, :] = t
        d = jnp.sum(t * knew[:, r // 8 * 128:r // 8 * 128 + 128], axis=1, keepdims=True)
        sn[r * 8:r * 8 + 8, :] = jnp.broadcast_to(d, (8, 128))
    slane = _iota((32, 128), 1) % 64 < 32
    for i in range(b):
        kwait(i)
        pos = lens[i] - 1 - base
        rows = [pl.ds(kp * 64 + i, 8, stride=8) for kp in range(4)]
        sc = jnp.concatenate([
            jnp.dot(qs[rows[kp], :].astype(BF16), kb[i, kp * 128:kp * 128 + 128, :], preferred_element_type=F32)
            for kp in range(4)], axis=0) * 0.125
        sc = jnp.where(_iota((32, s), 1) < pos, sc, -jnp.inf)
        new = jnp.concatenate([sn[rows[kp], :] for kp in range(4)], axis=0)[:, 0:1] * 0.125
        here = jnp.broadcast_to((pos >= 0) & (pos < s), new.shape)
        new = jnp.where(here, new, -jnp.inf)
        m = jnp.maximum(jnp.max(sc, axis=1, keepdims=True), new)
        safe = jnp.where(m == -jnp.inf, 0.0, m)
        p, pnew = jnp.exp(sc - safe), jnp.exp(new - safe)
        den = jnp.sum(p, axis=1, keepdims=True) + pnew
        ps[i] = p.astype(BF16)
        pn[i] = jnp.broadcast_to(pnew.astype(BF16).astype(F32), (32, 128))
        st[i] = jnp.where(slane, m, den)
    mine = _iota((8, 128), 0) // 4 == lane // 64
    for i in range(b):
        vwait(i)
        for grp in range(2):
            o = lax.dot_general(ps[i, grp * 16:grp * 16 + 16, :], vb[i, grp * 256:grp * 256 + 256, :],
                                (((1,), (1,)), ((), ())), preferred_element_type=F32)
            for half in range(2):
                kp = grp * 2 + half
                t = o[half * 8:half * 8 + 8, half * 128:half * 128 + 128]
                t = t + pn[i, kp * 8:kp * 8 + 8, :] * vnew[i:i + 1, kp * 128:kp * 128 + 128]
                v = jnp.where(mine, t, st[i, kp * 8:kp * 8 + 8, :])
                out[pl.ds(kp * 64 + i, 4, stride=8), :] = v[0:4]
                out[pl.ds(kp * 64 + 32 + i, 4, stride=8), :] = v[4:8]


class _Group:
    SCRATCH = (
        pltpu.VMEM((N, 32, 128), F32),
        pltpu.VMEM((2, 2, 8, HALF), F32),
        pltpu.VMEM((2, 2, 8, HALF), F32),
        pltpu.VMEM((2, 8, HALF), F32),
        pltpu.VMEM((2, 4, 8, HALF), F32),
        pltpu.VMEM((2, 2, 8, HALF), F32),
        DMA((N,)), DMA((N,)), DMA((2, 6)), DMA((2, 6)))

    def __init__(self, refs):
        (self.arecv, self.part, self.prec, self.csum, self.chips, self.hb,
         self.asend, self.aland, self.ssend, self.sland) = refs
        self.me = lax.axis_index('sp')
        self.sent = []

    def signal(self):
        self.barrier = pltpu.get_barrier_semaphore()
        for k in range(1, N):
            pl.semaphore_signal(self.barrier, inc=1, device_id={'sp': _peer(self.me, k)}, device_id_type=MESH)

    def enter(self):
        pl.semaphore_wait(self.barrier, N - 1)

    def send(self, src, dst, s0, s1, k):
        c = pltpu.make_async_remote_copy(src, dst, s0, s1, device_id={'sp': _peer(self.me, k)}, device_id_type=MESH)
        c.start()
        self.sent.append(c)
        return c

    def scatter(self, att):
        self.att = att
        self.parts = [
            self.send(att.at[pl.ds(pl.multiple_of(_peer(self.me, k) * 32, 32), 32), :], self.arecv.at[k],
                      self.asend.at[k], self.aland.at[k], k) for k in (7, 6, 5, 3, 4, 2, 1)]

    def combine(self):
        tiles = [self.att[pl.ds(pl.multiple_of(self.me * 32, 32), 32), :]]
        for c in self.parts:
            c.wait_recv()
        tiles += [self.arecv[k] for k in range(1, N)]
        low = _iota((32, 128), 1) % 64 < 32
        ms, ls = [], []
        for t in tiles:
            r = pltpu.roll(t, 64, 1)
            ms.append(jnp.where(low, r, pltpu.roll(r, 32, 1)))
            ls.append(jnp.where(low, pltpu.roll(r, 96, 1), r))
        top = functools.reduce(jnp.maximum, ms)
        num, den = jnp.zeros_like(top), jnp.zeros_like(top)
        for t, m, d in zip(tiles, ms, ls):
            c = jnp.exp(m - top)
            num, den = num + c * t, den + c * d
        o = num / den
        even = jnp.broadcast_to(self.me % 2 == 0, o.shape)
        o = jnp.where(even, o, pltpu.roll(o, 64, 1))
        other = pltpu.roll(o, 64, 1)
        first = _iota((8, 128), 1) < 64
        return jnp.concatenate([jnp.where(first, o[t * 16:t * 16 + 8], other[t * 16 + 8:t * 16 + 16])
                                for t in range(2)], axis=1).astype(BF16)

    def add(self, n, lhs, w, resid):
        me = self.me
        core, chip = me % 2, me // 2
        other = 1 - core

        def product(half):
            self.part[n, half] = jnp.dot(lhs, w[:, pl.ds(pl.multiple_of(half * HALF, HALF), HALF)],
                                         preferred_element_type=F32)

        def swap(half, i):
            return self.send(self.part.at[n, half], self.prec.at[n, half],
                             self.ssend.at[n, i], self.sland.at[n, i], 1)

        product(other)
        c0 = swap(other, 0)
        product(core)
        c1 = swap(core, 1)
        c0.wait_recv()
        self.csum[n] = self.part[n, core] + self.prec[n, core]
        hops = [self.send(self.csum.at[n], self.chips.at[n, chip], self.ssend.at[n, 1 + k // 2],
                          self.sland.at[n, 1 + k // 2], k) for k in (7, 5, 3)]
        c1.wait_recv()
        self.chips[n, chip] = self.part[n, other] + self.prec[n, other]
        for c in hops:
            c.wait_recv()
        t = self.chips
        self.hb[n, other] = resid(other) + ((t[n, 0] + t[n, 1]) + (t[n, 2] + t[n, 3]))
        c = self.send(self.hb.at[n, other], self.hb.at[n, other], self.ssend.at[n, 5], self.sland.at[n, 5], 1)
        c.wait_recv()

    def layer(self, h, g2, wo, w1, w2, xn, wait):
        lhs = self.combine()
        wait(0)
        self.add(0, lhs, wo, lambda half: h[:, pl.ds(pl.multiple_of(half * HALF, HALF), HALF)].astype(F32))
        hs = [self.hb[0, 0], self.hb[0, 1]]
        ss = sum(jnp.sum(x * x, axis=1, keepdims=True) for x in hs)
        r = lax.rsqrt(ss / (2 * HALF) + EPS)
        for c in range(2):
            xn[:, c * HALF:(c + 1) * HALF] = (hs[c] * r * g2[:, c * HALF:(c + 1) * HALF].astype(F32)).astype(BF16)
        wait(1)
        u = jax.nn.gelu(jnp.dot(xn[...], w1[...], preferred_element_type=F32)).astype(BF16)
        wait(2)
        self.add(1, u, w2, lambda half: self.hb[0, half])

    def leave(self):
        for c in self.sent:
            c.wait_send()


def _copies(pairs, sem):
    return [pltpu.make_async_copy(src, dst, sem.at[i]) for i, (src, dst) in enumerate(pairs)]


def _qkv_weights(l, wq, wk, wv, w, sem):
    return _copies([(wk.at[l], w.at[0]), (wv.at[l], w.at[1])]
                   + [(wq.at[l, :, pl.ds(512 * i, 512)], w.at[2 + i]) for i in range(4)], sem)


def _first(x, lens, g1, g2, wq, wk, wv, wo, w1, w2, kc, vc,
           h, new, kb0, vb0, kb1, vb1, wn,
           w, wob, w1b, w2b, qs, sn, ps, pn, st, att, xn, wsem, nsem, ksem, vsem, osem, csem, *group):
    grp = _Group(group)
    grp.signal()
    b, s = kb0.shape[0], kb0.shape[2]
    qkv = _qkv_weights(0, wq, wk, wv, w, wsem)
    kin = _copies([(kc.at[0, i], kb0.at[i]) for i in range(b)], ksem)
    vin = _copies([(vc.at[0, i], vb0.at[i]) for i in range(b)], vsem)
    rest = _copies([(wo.at[0], wob), (w1.at[0], w1b), (w2.at[0], w2b)], osem)
    for c in qkv + kin + vin + rest:
        c.start()
    proj = _project(x[...].astype(F32), g1[0:1, :].astype(F32), w, lambda i: qkv[i].wait())
    new[0], new[1] = proj[0], proj[1]
    _partials(proj, lens, grp.me * s, kb0, vb0, lambda i: kin[i].wait(), lambda i: vin[i].wait(),
              qs, sn, ps, pn, st, att)
    grp.enter()
    grp.scatter(att)
    ahead = _qkv_weights(1, wq, wk, wv, wn, nsem) + _copies([(kc.at[1], kb1), (vc.at[1], vb1)], csem)
    for c in ahead:
        c.start()
    grp.layer(x, g2[0:1, :], wob, w1b, w2b, xn, lambda i: rest[i].wait())
    for c in range(2):
        h[:, c * HALF:(c + 1) * HALF] = grp.hb[1, c]
    for c in ahead:
        c.wait()
    grp.leave()


def _second(h, lens, g1, new, kb0, vb0, kb1, vb1, w,
            att, ko, vo, qs, sn, ps, pn, st, cols, blocks, bsem, csem):
    b, s = kb0.shape[0], kb0.shape[2]
    base = lax.axis_index('sp') * s
    caches = [(kb0, ko, 0), (vb0, vo, 0), (kb1, ko, 1), (vb1, vo, 1)]
    bulk = [pltpu.make_async_copy(src.at[i], dst.at[l, i], bsem.at[n, i])
            for n, (src, dst, l) in enumerate(caches) for i in range(b)]
    for c in bulk:
        c.start()
    proj = _project(h[...], g1[1:2, :].astype(F32), w, lambda i: None)
    _partials(proj, lens, base, kb1, vb1, lambda i: None, lambda i: None, qs, sn, ps, pn, st, att)
    for n, x in enumerate((new[0], new[1], proj[0], proj[1])):
        cols[n] = jnp.broadcast_to(x[:, None, :], (b, 16, s)).reshape(b * 16, s).T

    def each(n, i, do):
        src, dst, l = caches[n]
        pos = lens[i] - 1 - base

        @pl.when((pos >= 0) & (pos < s))
        def _():
            at = pl.ds(pl.multiple_of(pos // 128 * 128, 128), 128)
            do(src, pos, at, pltpu.make_async_copy(blocks.at[n, i], dst.at[l, i, :, at], csem.at[n, i]),
               bulk[n * b + i])

        return (pos >= 0) & (pos < s)

    def fill(n, i):
        def do(src, pos, at, c, whole):
            hit = _iota((s, 128), 1) == pos % 128
            col = cols[n, :, i * 16:i * 16 + 1]
            blocks[n, i] = jnp.where(hit, col, src[i, :, at].astype(F32)).astype(BF16)
            whole.wait()
            c.start()

        here = each(n, i, do)

        @pl.when(jnp.logical_not(here))
        def _():
            bulk[n * b + i].wait()

    for n in range(4):
        for i in range(b):
            fill(n, i)
    for n in range(4):
        for i in range(b):
            each(n, i, lambda src, pos, at, c, whole: c.wait())


def _third(h, att, g2, wo, w1, w2, y, wob, w1b, w2b, xn, osem, *group):
    grp = _Group(group)
    grp.signal()
    rest = _copies([(wo.at[1], wob), (w1.at[1], w1b), (w2.at[1], w2b)], osem)
    for c in rest:
        c.start()
    grp.enter()
    grp.scatter(att)
    grp.layer(h, g2[1:2, :], wob, w1b, w2b, xn, lambda i: rest[i].wait())
    for c in range(2):
        y[:, c * HALF:(c + 1) * HALF] = grp.hb[1, c].astype(y.dtype)
    grp.leave()


def solution(mesh):
    kspec = P(None, 'dp', 'sp', None, None)

    def local(x, lens, wq, wk, wv, wo, w1, w2, g1, g2, kc, vc):
        nl, b, s, kvh, dh = kc.shape
        d = kvh * dh
        kt = kc.transpose(0, 1, 3, 4, 2).reshape(nl, b, d, s)
        vt = vc.transpose(0, 1, 3, 4, 2).reshape(nl, b, d, s)
        slice_, weights = pltpu.VMEM((b, d, s), BF16), pltpu.VMEM((6, wq.shape[1], d), BF16)
        mlp = [pltpu.VMEM(w.shape[1:], BF16) for w in (wo, w1, w2)]
        local_ = [pltpu.VMEM((256, 128), F32), pltpu.VMEM((256, 128), F32), pltpu.VMEM((b, 32, s), BF16),
                  pltpu.VMEM((b, 32, 128), F32), pltpu.VMEM((b, 32, 128), F32)]
        partial = pltpu.VMEM((256, 128), F32)
        rows = pltpu.VMEM(x.shape, BF16)

        def call(body, name, n_in, out_shape, out_specs, scratch, collective_id=None, limit=64):
            return pl.pallas_call(
                body, out_shape=out_shape, in_specs=n_in, out_specs=out_specs, scratch_shapes=scratch,
                compiler_params=pltpu.CompilerParams(
                    collective_id=collective_id, has_side_effects=collective_id is not None,
                    vmem_limit_bytes=limit << 20), name=name)

        h, new, *held = call(
            _first, 'first', [VMEM, SMEM, VMEM, VMEM] + [HBM] * 8,
            (pltpu.VMEM(x.shape, F32), pltpu.VMEM((2, b, d), F32), slice_, slice_, slice_, slice_, weights),
            (VMEM,) * 7,
            [weights, *mlp, *local_, partial, rows,
             DMA((6,)), DMA((6,)), DMA((b,)), DMA((b,)), DMA((3,)), DMA((2,)), *_Group.SCRATCH], 0, limit=28,
        )(x, lens, g1, g2, *_in(pltpu.HBM, wq, wk, wv, wo, w1, w2, kt, vt))
        cache = jax.ShapeDtypeStruct(kt.shape, kt.dtype)
        att, ko, vo = call(
            _second, 'second', [VMEM, SMEM, VMEM] + [VMEM] * 6, (pltpu.VMEM((256, 128), F32), cache, cache),
            (VMEM, HBM, HBM),
            [*local_, pltpu.VMEM((4, s, 128), F32), pltpu.VMEM((4, b, d, 128), BF16), DMA((4, b)), DMA((4, b))], limit=14,
        )(h, lens, g1, *_in(pltpu.VMEM, new, *held))
        y = call(
            _third, 'third', [VMEM, VMEM, VMEM] + [HBM] * 3, jax.ShapeDtypeStruct(x.shape, BF16), VMEM,
            [*mlp, rows, DMA((3,)), *_Group.SCRATCH], 1, limit=16,
        )(h, att, g2, *_in(pltpu.HBM, wo, w1, w2))
        back = [t.reshape(nl, b, kvh, dh, s).transpose(0, 1, 4, 2, 3) for t in (ko, vo)]
        return y, *back

    return jax.shard_map(
        local, mesh=mesh,
        in_specs=(P('dp', None), P('dp'), P(), P(), P(), P(None, 'sp', None), P(None, None, 'sp'),
                  P(None, 'sp', None), P(), P(), kspec, kspec),
        out_specs=(P('dp', None), kspec, kspec), check_vma=False)
```

```python
import functools

import jax
import jax.numpy as jnp
from jax import lax
from jax.experimental import pallas as pl
from jax.experimental.pallas import tpu as pltpu
from jax.sharding import PartitionSpec as P

EPS = 1e-6
F32 = jnp.float32
BF16 = jnp.bfloat16
MESH = pl.DeviceIdType.MESH
HBM = pl.BlockSpec(memory_space=pl.ANY)
VMEM = pl.BlockSpec(memory_space=pltpu.VMEM)
SMEM = pl.BlockSpec(memory_space=pltpu.SMEM)
DMA = pltpu.SemaphoreType.DMA
N = 8
HALF = 1024


def _in(space, *arrays):
    return [pltpu.with_memory_space_constraint(a, space) for a in arrays]


def _iota(shape, dim):
    return lax.broadcasted_iota(jnp.int32, shape, dim)


def _peer(me, k):
    y, x, c = me // 4, me // 2 % 2, me % 2
    return (y + k // 4) % 2 * 4 + (x + k // 2 % 2) % 2 * 2 + (c + k % 2) % 2


def _project(h, g, w, wait):
    r = lax.rsqrt(jnp.mean(h * h, axis=-1, keepdims=True) + EPS)
    xn = (h * r * g).astype(BF16)
    out = []
    for i in range(w.shape[0]):
        wait(i)
        out.append(jnp.dot(xn, w[i], preferred_element_type=F32).astype(BF16).astype(F32))
    return out


def _partials(proj, lens, base, kb, vb, kwait, vwait, qs, sn, ps, pn, st, out):
    knew, vnew = proj[0], proj[1]
    b, s = kb.shape[0], kb.shape[2]
    lane = _iota((8, 128), 1)
    for r in range(32):
        t = proj[2 + r // 8][:, (r // 2 % 4) * 128:(r // 2 % 4) * 128 + 128]
        half = r // 4 % 2
        if r % 2 != half:
            t = pltpu.roll(t, 64, 1)
        t = jnp.where(lane // 64 == half, t, 0.0)
        qs[r * 8:r * 8 + 8, :] = t
        d = jnp.sum(t * knew[:, r // 8 * 128:r // 8 * 128 + 128], axis=1, keepdims=True)
        sn[r * 8:r * 8 + 8, :] = jnp.broadcast_to(d, (8, 128))
    slane = _iota((32, 128), 1) % 64 < 32
    kwait()
    for i in range(b):
        pos = lens[i] - 1 - base
        rows = [pl.ds(kp * 64 + i, 8, stride=8) for kp in range(4)]
        sc = jnp.concatenate([
            jnp.dot(qs[rows[kp], :].astype(BF16), kb[i, kp * 128:kp * 128 + 128, :], preferred_element_type=F32)
            for kp in range(4)], axis=0) * 0.125
        sc = jnp.where(_iota((32, s), 1) < pos, sc, -jnp.inf)
        new = jnp.concatenate([sn[rows[kp], :] for kp in range(4)], axis=0)[:, 0:1] * 0.125
        here = jnp.broadcast_to((pos >= 0) & (pos < s), new.shape)
        new = jnp.where(here, new, -jnp.inf)
        m = jnp.maximum(jnp.max(sc, axis=1, keepdims=True), new)
        safe = jnp.where(m == -jnp.inf, 0.0, m)
        p, pnew = jnp.exp(sc - safe), jnp.exp(new - safe)
        den = jnp.sum(p, axis=1, keepdims=True) + pnew
        ps[i] = p.astype(BF16)
        pn[i] = jnp.broadcast_to(pnew.astype(BF16).astype(F32), (32, 128))
        st[i] = jnp.where(slane, m, den)
    mine = _iota((8, 128), 0) // 4 == lane // 64
    vwait()
    for i in range(b):
        for grp in range(2):
            o = lax.dot_general(ps[i, grp * 16:grp * 16 + 16, :], vb[i, grp * 256:grp * 256 + 256, :],
                                (((1,), (1,)), ((), ())), preferred_element_type=F32)
            for half in range(2):
                kp = grp * 2 + half
                t = o[half * 8:half * 8 + 8, half * 128:half * 128 + 128]
                t = t + pn[i, kp * 8:kp * 8 + 8, :] * vnew[i:i + 1, kp * 128:kp * 128 + 128]
                v = jnp.where(mine, t, st[i, kp * 8:kp * 8 + 8, :])
                out[pl.ds(kp * 64 + i, 4, stride=8), :] = v[0:4]
                out[pl.ds(kp * 64 + 32 + i, 4, stride=8), :] = v[4:8]


class _Group:
    SCRATCH = (
        pltpu.VMEM((N, 32, 128), F32),
        pltpu.VMEM((2, 2, 8, HALF), F32),
        pltpu.VMEM((2, 2, 8, HALF), F32),
        pltpu.VMEM((2, 8, HALF), F32),
        pltpu.VMEM((2, 4, 8, HALF), F32),
        pltpu.VMEM((2, 2, 8, HALF), F32),
        DMA((N,)), DMA((N,)), DMA((2, 6)), DMA((2, 6)))

    def __init__(self, refs):
        (self.arecv, self.part, self.prec, self.csum, self.chips, self.hb,
         self.asend, self.aland, self.ssend, self.sland) = refs
        self.me = lax.axis_index('sp')
        self.sent = []

    def signal(self):
        self.barrier = pltpu.get_barrier_semaphore()
        for k in range(1, N):
            pl.semaphore_signal(self.barrier, inc=1, device_id={'sp': _peer(self.me, k)}, device_id_type=MESH)

    def enter(self):
        pl.semaphore_wait(self.barrier, N - 1)

    def send(self, src, dst, s0, s1, k):
        c = pltpu.make_async_remote_copy(src, dst, s0, s1, device_id={'sp': _peer(self.me, k)}, device_id_type=MESH)
        c.start()
        self.sent.append(c)
        return c

    def scatter(self, att):
        self.att = att
        self.parts = [
            self.send(att.at[pl.ds(pl.multiple_of(_peer(self.me, k) * 32, 32), 32), :], self.arecv.at[k],
                      self.asend.at[k], self.aland.at[k], k) for k in (7, 6, 5, 3, 4, 2, 1)]

    def combine(self):
        tiles = [self.att[pl.ds(pl.multiple_of(self.me * 32, 32), 32), :]]
        for c in self.parts:
            c.wait_recv()
        tiles += [self.arecv[k] for k in range(1, N)]
        low = _iota((32, 128), 1) % 64 < 32
        ms, ls = [], []
        for t in tiles:
            r = pltpu.roll(t, 64, 1)
            ms.append(jnp.where(low, r, pltpu.roll(r, 32, 1)))
            ls.append(jnp.where(low, pltpu.roll(r, 96, 1), r))
        top = functools.reduce(jnp.maximum, ms)
        num, den = jnp.zeros_like(top), jnp.zeros_like(top)
        for t, m, d in zip(tiles, ms, ls):
            c = jnp.exp(m - top)
            num, den = num + c * t, den + c * d
        o = num / den
        even = jnp.broadcast_to(self.me % 2 == 0, o.shape)
        o = jnp.where(even, o, pltpu.roll(o, 64, 1))
        other = pltpu.roll(o, 64, 1)
        first = _iota((8, 128), 1) < 64
        return jnp.concatenate([jnp.where(first, o[t * 16:t * 16 + 8], other[t * 16 + 8:t * 16 + 16])
                                for t in range(2)], axis=1).astype(BF16)

    def add(self, n, lhs, w, resid):
        me = self.me
        core, chip = me % 2, me // 2
        other = 1 - core

        def product(half):
            self.part[n, half] = jnp.dot(lhs, w[:, pl.ds(pl.multiple_of(half * HALF, HALF), HALF)],
                                         preferred_element_type=F32)

        def swap(half, i):
            return self.send(self.part.at[n, half], self.prec.at[n, half],
                             self.ssend.at[n, i], self.sland.at[n, i], 1)

        product(other)
        c0 = swap(other, 0)
        product(core)
        c1 = swap(core, 1)
        c0.wait_recv()
        self.csum[n] = self.part[n, core] + self.prec[n, core]
        hops = [self.send(self.csum.at[n], self.chips.at[n, chip], self.ssend.at[n, 1 + k // 2],
                          self.sland.at[n, 1 + k // 2], k) for k in (7, 5, 3)]
        c1.wait_recv()
        self.chips[n, chip] = self.part[n, other] + self.prec[n, other]
        for c in hops:
            c.wait_recv()
        t = self.chips
        self.hb[n, other] = resid(other) + ((t[n, 0] + t[n, 1]) + (t[n, 2] + t[n, 3]))
        c = self.send(self.hb.at[n, other], self.hb.at[n, other], self.ssend.at[n, 5], self.sland.at[n, 5], 1)
        c.wait_recv()

    def layer(self, h, g2, wo, w1, w2, xn, wait):
        lhs = self.combine()
        wait(0)
        self.add(0, lhs, wo, lambda half: h[:, pl.ds(pl.multiple_of(half * HALF, HALF), HALF)].astype(F32))
        hs = [self.hb[0, 0], self.hb[0, 1]]
        ss = sum(jnp.sum(x * x, axis=1, keepdims=True) for x in hs)
        r = lax.rsqrt(ss / (2 * HALF) + EPS)
        for c in range(2):
            xn[:, c * HALF:(c + 1) * HALF] = (hs[c] * r * g2[:, c * HALF:(c + 1) * HALF].astype(F32)).astype(BF16)
        wait(1)
        u = jax.nn.gelu(jnp.dot(xn[...], w1[...], preferred_element_type=F32)).astype(BF16)
        wait(2)
        self.add(1, u, w2, lambda half: self.hb[0, half])

    def leave(self):
        for c in self.sent:
            c.wait_send()


def _copies(pairs, sem):
    return [pltpu.make_async_copy(src, dst, sem.at[i]) for i, (src, dst) in enumerate(pairs)]


def _start(copies):
    for c in copies:
        c.start()


def _wait(copies):
    for c in copies:
        c.wait()


def _qkv_weights(l, wq, wk, wv, w, sem):
    return _copies([(wk.at[l], w.at[0]), (wv.at[l], w.at[1])]
                   + [(wq.at[l, :, pl.ds(512 * i, 512)], w.at[2 + i]) for i in range(4)], sem)


def _first(x_, lens_, g1_, g2_, wq, wk, wv, wo, w1, w2, kc, vc,
           h, new, kb0, vb0, kb1, vb1, wn,
           w, wob, w1b, w2b, qs, sn, ps, pn, st, att, xn, wsem, nsem, ksem, vsem, osem, csem,
           x, lens, g1, g2, msem, pr, psem, *group):
    small = _copies([(x_, x), (g1_, g1), (lens_, lens), (g2_, g2)], msem)
    for c in small:
        c.start()
    grp = _Group(group)
    grp.signal()
    b, s = kb0.shape[0], kb0.shape[2]
    core = grp.me % 2
    rows = w.shape[1]

    def pieces(src, i, n, start):
        return [pltpu.make_async_copy(src.at[pl.ds(j * rows // n, rows // n), :],
                                      w.at[i, pl.ds(j * rows // n, rows // n), :], wsem.at[start + j])
                for j in range(n)]

    @pl.when(core == 0)
    def _():
        _start(pieces(wk.at[0], 0, 8, 0))

    @pl.when(core == 1)
    def _():
        _start(pieces(wv.at[0], 0, 8, 0))

    quarter = [wq.at[0, :, pl.ds(pl.multiple_of(core * 1024 + 512 * i, 512), 512)] for i in range(2)]
    qkv = [pieces(wk.at[0], 0, 8, 0), pieces(quarter[0], 1, 4, 8), pieces(quarter[1], 2, 4, 12)]
    kin = _copies([(kc.at[0, i], kb0.at[i]) for i in range(b)], ksem)
    vin = _copies([(vc.at[0, pl.ds(2 * i, 2)], vb0.at[pl.ds(2 * i, 2)]) for i in range(b // 2)], vsem)
    rest = _copies([(wo.at[0], wob), (w1.at[0], w1b), (w2.at[0], w2b)], osem)
    _start(qkv[1] + qkv[2])
    _wait(small)
    grp.enter()

    def arrived(i):
        _wait(qkv[i])
        if i == 1:
            _start(kin)
        if i == 2:
            _start(vin)

    mine = _project(x[...].astype(F32), g1[0:1, :].astype(F32), w, arrived)
    for i in range(3):
        pr[core, i] = mine[i].astype(BF16)
    c = grp.send(pr.at[core], pr.at[core], psem.at[0], psem.at[1], 1)
    c.wait_recv()
    proj = [pr[0, 0], pr[1, 0], pr[0, 1], pr[0, 2], pr[1, 1], pr[1, 2]]
    proj = [t.astype(F32) for t in proj]
    new[0], new[1] = proj[0], proj[1]
    _partials(proj, lens, grp.me * s, kb0, vb0, lambda: _wait(kin), lambda: _wait(vin),
              qs, sn, ps, pn, st, att)
    grp.scatter(att)
    ahead = _qkv_weights(1, wq, wk, wv, wn, nsem) + _copies([(kc.at[1], kb1), (vc.at[1], vb1)], csem)
    for c in rest + ahead:
        c.start()
    grp.layer(x, g2[0:1, :], wob, w1b, w2b, xn, lambda i: rest[i].wait())
    for c in range(2):
        h[:, c * HALF:(c + 1) * HALF] = grp.hb[1, c]
    for c in ahead:
        c.wait()
    grp.leave()


def _second(h, lens, g1, new, kb0, vb0, kb1, vb1, w,
            att, ko, vo, qs, sn, ps, pn, st, cols, blocks, bsem, csem):
    b, s = kb0.shape[0], kb0.shape[2]
    base = lax.axis_index('sp') * s
    caches = [(kb0, ko, 0), (vb0, vo, 0), (kb1, ko, 1), (vb1, vo, 1)]
    bulk = [pltpu.make_async_copy(src.at[i], dst.at[l, i], bsem.at[n, i])
            for n, (src, dst, l) in enumerate(caches) for i in range(b)]

    @pl.loop(0, b)
    def _(i):
        for n, (src, dst, l) in enumerate(caches):
            pltpu.make_async_copy(src.at[i], dst.at[l, i], bsem.at[n, i]).start()

    proj = _project(h[...], g1[1:2, :].astype(F32), w, lambda i: None)
    _partials(proj, lens, base, kb1, vb1, lambda: None, lambda: None, qs, sn, ps, pn, st, att)
    for n, x in enumerate((new[0], new[1], proj[0], proj[1])):
        cols[n] = jnp.broadcast_to(x[:, None, :], (b, 16, s)).reshape(b * 16, s).T

    def owned(i, do):
        pos = lens[i] - 1 - base

        @pl.when((pos >= 0) & (pos < s))
        def _():
            at = pl.ds(pl.multiple_of(pos // 128 * 128, 128), 128)
            for n, (src, dst, l) in enumerate(caches):
                do(n, src, pos, at, pltpu.make_async_copy(blocks.at[n, i], dst.at[l, i, :, at], csem.at[n, i]))

    def fill(i):
        def do(n, src, pos, at, c):
            hit = _iota((s, 128), 1) == pos % 128
            blocks[n, i] = jnp.where(hit, cols[n, :, i * 16:i * 16 + 1], src[i, :, at].astype(F32)).astype(BF16)
        owned(i, do)

    for i in range(b):
        fill(i)
    _wait(bulk)
    for i in range(b):
        owned(i, lambda n, src, pos, at, c: c.start())
    for i in range(b):
        owned(i, lambda n, src, pos, at, c: c.wait())


def _third(h, att, g2, wo, w1, w2, y, wob, w1b, w2b, xn, osem, *group):
    grp = _Group(group)
    grp.signal()
    rest = _copies([(wo.at[1], wob), (w1.at[1], w1b), (w2.at[1], w2b)], osem)
    for c in rest:
        c.start()
    grp.enter()
    grp.scatter(att)
    grp.layer(h, g2[1:2, :], wob, w1b, w2b, xn, lambda i: rest[i].wait())
    for c in range(2):
        y[:, c * HALF:(c + 1) * HALF] = grp.hb[1, c].astype(y.dtype)
    grp.leave()


def solution(mesh):
    kspec = P(None, 'dp', 'sp', None, None)

    def local(x, lens, wq, wk, wv, wo, w1, w2, g1, g2, kc, vc):
        nl, b, s, kvh, dh = kc.shape
        d = kvh * dh
        kt = kc.transpose(0, 1, 3, 4, 2).reshape(nl, b, d, s)
        vt = vc.transpose(0, 1, 3, 4, 2).reshape(nl, b, d, s)
        slice_, weights = pltpu.VMEM((b, d, s), BF16), pltpu.VMEM((6, wq.shape[1], d), BF16)
        mlp = [pltpu.VMEM(w.shape[1:], BF16) for w in (wo, w1, w2)]
        local_ = [pltpu.VMEM((256, 128), F32), pltpu.VMEM((256, 128), F32), pltpu.VMEM((b, 32, s), BF16),
                  pltpu.VMEM((b, 32, 128), F32), pltpu.VMEM((b, 32, 128), F32)]
        partial = pltpu.VMEM((256, 128), F32)
        rows = pltpu.VMEM(x.shape, BF16)

        def call(body, name, n_in, out_shape, out_specs, scratch, collective_id=None, limit=64):
            return pl.pallas_call(
                body, out_shape=out_shape, in_specs=n_in, out_specs=out_specs, scratch_shapes=scratch,
                compiler_params=pltpu.CompilerParams(
                    collective_id=collective_id, has_side_effects=collective_id is not None,
                    vmem_limit_bytes=limit << 20), name=name)

        h, new, *held = call(
            _first, 'first', [HBM] * 12,
            (pltpu.VMEM(x.shape, F32), pltpu.VMEM((2, b, d), F32), slice_, slice_, slice_, slice_, weights),
            (VMEM,) * 7,
            [pltpu.VMEM((3, wq.shape[1], d), BF16), *mlp, *local_, partial, rows,
             DMA((16,)), DMA((6,)), DMA((b,)), DMA((b,)), DMA((3,)), DMA((2,)),
             rows, pltpu.SMEM(lens.shape, lens.dtype), pltpu.VMEM(g1.shape, BF16), pltpu.VMEM(g2.shape, BF16), DMA((4,)),
             pltpu.VMEM((2, 3, b, d), BF16), DMA((2,)),
             *_Group.SCRATCH], 0, limit=22,
        )(*_in(pltpu.HBM, x, lens, g1, g2, wq, wk, wv, wo, w1, w2, kt, vt))
        cache = jax.ShapeDtypeStruct(kt.shape, kt.dtype)
        att, ko, vo = call(
            _second, 'second', [VMEM, SMEM, VMEM] + [VMEM] * 6, (pltpu.VMEM((256, 128), F32), cache, cache),
            (VMEM, HBM, HBM),
            [*local_, pltpu.VMEM((4, s, 128), F32), pltpu.VMEM((4, b, d, 128), BF16), DMA((4, b)), DMA((4, b))], limit=14,
        )(h, lens, g1, *_in(pltpu.VMEM, new, *held))
        y = call(
            _third, 'third', [VMEM, VMEM, VMEM] + [HBM] * 3, jax.ShapeDtypeStruct(x.shape, BF16), VMEM,
            [*mlp, rows, DMA((3,)), *_Group.SCRATCH], 1, limit=16,
        )(h, att, g2, *_in(pltpu.HBM, wo, w1, w2))
        back = [t.reshape(nl, b, kvh, dh, s).transpose(0, 1, 4, 2, 3) for t in (ko, vo)]
        return y, *back

    return jax.shard_map(
        local, mesh=mesh,
        in_specs=(P('dp', None), P('dp'), P(), P(), P(), P(None, 'sp', None), P(None, None, 'sp'),
                  P(None, 'sp', None), P(), P(), kspec, kspec),
        out_specs=(P('dp', None), kspec, kspec), check_vma=False)
```

```python
import functools

import jax
import jax.numpy as jnp
from jax import lax
from jax.experimental import pallas as pl
from jax.experimental.pallas import tpu as pltpu
from jax.sharding import PartitionSpec as P

EPS = 1e-6
F32 = jnp.float32
BF16 = jnp.bfloat16
MESH = pl.DeviceIdType.MESH
HBM = pl.BlockSpec(memory_space=pl.ANY)
VMEM = pl.BlockSpec(memory_space=pltpu.VMEM)
SMEM = pl.BlockSpec(memory_space=pltpu.SMEM)
DMA = pltpu.SemaphoreType.DMA
N = 8
HALF = 1024


def _in(space, *arrays):
    return [pltpu.with_memory_space_constraint(a, space) for a in arrays]


def _iota(shape, dim):
    return lax.broadcasted_iota(jnp.int32, shape, dim)


def _peer(me, k):
    y, x, c = me // 4, me // 2 % 2, me % 2
    return (y + k // 4) % 2 * 4 + (x + k // 2 % 2) % 2 * 2 + (c + k % 2) % 2


def _project(h, g, w, wait):
    r = lax.rsqrt(jnp.mean(h * h, axis=-1, keepdims=True) + EPS)
    xn = (h * r * g).astype(BF16)
    out = []
    for i in range(w.shape[0]):
        wait(i)
        out.append(jnp.dot(xn, w[i], preferred_element_type=F32).astype(BF16).astype(F32))
    return out


def _partials(proj, lens, base, kb, vb, kwait, vwait, qs, sn, ps, pn, st, out):
    knew, vnew = proj[0], proj[1]
    b, s = kb.shape[0], kb.shape[2]
    lane = _iota((8, 128), 1)
    for r in range(32):
        t = proj[2 + r // 8][:, (r // 2 % 4) * 128:(r // 2 % 4) * 128 + 128]
        half = r // 4 % 2
        if r % 2 != half:
            t = pltpu.roll(t, 64, 1)
        t = jnp.where(lane // 64 == half, t, 0.0)
        qs[r * 8:r * 8 + 8, :] = t
        d = jnp.sum(t * knew[:, r // 8 * 128:r // 8 * 128 + 128], axis=1, keepdims=True)
        sn[r * 8:r * 8 + 8, :] = jnp.broadcast_to(d, (8, 128))
    slane = _iota((32, 128), 1) % 64 < 32
    kwait()
    for i in range(b):
        pos = lens[i] - 1 - base
        rows = [pl.ds(kp * 64 + i, 8, stride=8) for kp in range(4)]
        sc = jnp.concatenate([
            jnp.dot(qs[rows[kp], :].astype(BF16), kb[i, kp * 128:kp * 128 + 128, :], preferred_element_type=F32)
            for kp in range(4)], axis=0) * 0.125
        sc = jnp.where(_iota((32, s), 1) < pos, sc, -jnp.inf)
        new = jnp.concatenate([sn[rows[kp], :] for kp in range(4)], axis=0)[:, 0:1] * 0.125
        here = jnp.broadcast_to((pos >= 0) & (pos < s), new.shape)
        new = jnp.where(here, new, -jnp.inf)
        m = jnp.maximum(jnp.max(sc, axis=1, keepdims=True), new)
        safe = jnp.where(m == -jnp.inf, 0.0, m)
        p, pnew = jnp.exp(sc - safe), jnp.exp(new - safe)
        den = jnp.sum(p, axis=1, keepdims=True) + pnew
        ps[i] = p.astype(BF16)
        pn[i] = jnp.broadcast_to(pnew.astype(BF16).astype(F32), (32, 128))
        st[i] = jnp.where(slane, m, den)
    mine = _iota((8, 128), 0) // 4 == lane // 64
    vwait()
    for i in range(b):
        for grp in range(2):
            o = lax.dot_general(ps[i, grp * 16:grp * 16 + 16, :], vb[i, grp * 256:grp * 256 + 256, :],
                                (((1,), (1,)), ((), ())), preferred_element_type=F32)
            for half in range(2):
                kp = grp * 2 + half
                t = o[half * 8:half * 8 + 8, half * 128:half * 128 + 128]
                t = t + pn[i, kp * 8:kp * 8 + 8, :] * vnew[i:i + 1, kp * 128:kp * 128 + 128]
                v = jnp.where(mine, t, st[i, kp * 8:kp * 8 + 8, :])
                out[pl.ds(kp * 64 + i, 4, stride=8), :] = v[0:4]
                out[pl.ds(kp * 64 + 32 + i, 4, stride=8), :] = v[4:8]


class _Group:
    SCRATCH = (
        pltpu.VMEM((N, 32, 128), F32),
        pltpu.VMEM((2, 2, 8, HALF), F32),
        pltpu.VMEM((2, 2, 8, HALF), F32),
        pltpu.VMEM((2, 8, HALF), F32),
        pltpu.VMEM((2, 4, 8, HALF), F32),
        pltpu.VMEM((2, 2, 8, HALF), F32),
        DMA((N,)), DMA((N,)), DMA((2, 6)), DMA((2, 6)))

    def __init__(self, refs):
        (self.arecv, self.part, self.prec, self.csum, self.chips, self.hb,
         self.asend, self.aland, self.ssend, self.sland) = refs
        self.me = lax.axis_index('sp')
        self.sent = []

    def signal(self):
        self.barrier = pltpu.get_barrier_semaphore()
        for k in range(1, N):
            pl.semaphore_signal(self.barrier, inc=1, device_id={'sp': _peer(self.me, k)}, device_id_type=MESH)

    def enter(self):
        pl.semaphore_wait(self.barrier, N - 1)

    def send(self, src, dst, s0, s1, k):
        c = pltpu.make_async_remote_copy(src, dst, s0, s1, device_id={'sp': _peer(self.me, k)}, device_id_type=MESH)
        c.start()
        self.sent.append(c)
        return c

    def scatter(self, att):
        self.att = att
        self.parts = [
            self.send(att.at[pl.ds(pl.multiple_of(_peer(self.me, k) * 32, 32), 32), :], self.arecv.at[k],
                      self.asend.at[k], self.aland.at[k], k) for k in (7, 6, 5, 3, 4, 2, 1)]

    def combine(self):
        tiles = [self.att[pl.ds(pl.multiple_of(self.me * 32, 32), 32), :]]
        for c in self.parts:
            c.wait_recv()
        tiles += [self.arecv[k] for k in range(1, N)]
        low = _iota((32, 128), 1) % 64 < 32
        ms, ls = [], []
        for t in tiles:
            r = pltpu.roll(t, 64, 1)
            ms.append(jnp.where(low, r, pltpu.roll(r, 32, 1)))
            ls.append(jnp.where(low, pltpu.roll(r, 96, 1), r))
        top = functools.reduce(jnp.maximum, ms)
        num, den = jnp.zeros_like(top), jnp.zeros_like(top)
        for t, m, d in zip(tiles, ms, ls):
            c = jnp.exp(m - top)
            num, den = num + c * t, den + c * d
        o = num / den
        even = jnp.broadcast_to(self.me % 2 == 0, o.shape)
        o = jnp.where(even, o, pltpu.roll(o, 64, 1))
        other = pltpu.roll(o, 64, 1)
        first = _iota((8, 128), 1) < 64
        return jnp.concatenate([jnp.where(first, o[t * 16:t * 16 + 8], other[t * 16 + 8:t * 16 + 16])
                                for t in range(2)], axis=1).astype(BF16)

    def add(self, n, lhs, w, resid):
        me = self.me
        core, chip = me % 2, me // 2
        other = 1 - core

        def swap(i):
            half = (other + i) % 2
            return pltpu.make_async_remote_copy(
                self.part.at[n, half], self.prec.at[n, half], self.ssend.at[n, i], self.sland.at[n, i],
                device_id={'sp': _peer(me, 1)}, device_id_type=MESH)

        for i in range(2):
            half = (other + i) % 2
            self.part[n, half] = jnp.dot(lhs, w[:, pl.ds(pl.multiple_of(half * HALF, HALF), HALF)],
                                         preferred_element_type=F32)
            swap(i).start()

        c0, c1 = swap(0), swap(1)
        self.sent += [c0, c1]
        c0.wait_recv()
        self.csum[n] = self.part[n, core] + self.prec[n, core]
        hops = [self.send(self.csum.at[n], self.chips.at[n, chip], self.ssend.at[n, 1 + k // 2],
                          self.sland.at[n, 1 + k // 2], k) for k in (7, 5, 3)]
        c1.wait_recv()
        self.chips[n, chip] = self.part[n, other] + self.prec[n, other]
        for c in hops:
            c.wait_recv()
        t = self.chips
        self.hb[n, other] = resid(other) + ((t[n, 0] + t[n, 1]) + (t[n, 2] + t[n, 3]))
        c = self.send(self.hb.at[n, other], self.hb.at[n, other], self.ssend.at[n, 5], self.sland.at[n, 5], 1)
        c.wait_recv()

    def layer(self, h, g2, wo, w1, w2, xn, wait):
        lhs = self.combine()
        wait(0)
        self.add(0, lhs, wo, lambda half: h[:, pl.ds(pl.multiple_of(half * HALF, HALF), HALF)].astype(F32))
        hs = [self.hb[0, 0], self.hb[0, 1]]
        ss = sum(jnp.sum(x * x, axis=1, keepdims=True) for x in hs)
        r = lax.rsqrt(ss / (2 * HALF) + EPS)
        for c in range(2):
            xn[:, c * HALF:(c + 1) * HALF] = (hs[c] * r * g2[:, c * HALF:(c + 1) * HALF].astype(F32)).astype(BF16)
        wait(1)
        u = jax.nn.gelu(jnp.dot(xn[...], w1[...], preferred_element_type=F32)).astype(BF16)
        wait(2)
        self.add(1, u, w2, lambda half: self.hb[0, half])

    def leave(self):
        for c in self.sent:
            c.wait_send()


def _copies(pairs, sem):
    return [pltpu.make_async_copy(src, dst, sem.at[i]) for i, (src, dst) in enumerate(pairs)]


def _start(copies):
    for c in copies:
        c.start()


def _wait(copies):
    for c in copies:
        c.wait()


def _qkv_weights(l, wq, wk, wv, w, sem):
    return _copies([(wk.at[l], w.at[0]), (wv.at[l], w.at[1])]
                   + [(wq.at[l, :, pl.ds(512 * i, 512)], w.at[2 + i]) for i in range(4)], sem)


def _first(x_, lens_, g1_, g2_, wq, wk, wv, wo, w1, w2, kc, vc,
           h, new, kb0, vb0, kb1, vb1, wn,
           w, wob, w1b, w2b, qs, sn, ps, pn, st, att, xn, wsem, nsem, ksem, vsem, osem, csem,
           x, lens, g1, g2, msem, pr, psem, *group):
    small = _copies([(x_, x), (g1_, g1), (lens_, lens), (g2_, g2)], msem)
    for c in small:
        c.start()
    grp = _Group(group)
    grp.signal()
    b, s = kb0.shape[0], kb0.shape[2]
    core = grp.me % 2
    rows = w.shape[1]

    def pieces(src, i, n, start):
        return [pltpu.make_async_copy(src.at[pl.ds(j * rows // n, rows // n), :],
                                      w.at[i, pl.ds(j * rows // n, rows // n), :], wsem.at[start + j])
                for j in range(n)]

    @pl.when(core == 0)
    def _():
        _start(pieces(wk.at[0], 0, 8, 0))

    @pl.when(core == 1)
    def _():
        _start(pieces(wv.at[0], 0, 8, 0))

    quarter = [wq.at[0, :, pl.ds(pl.multiple_of(core * 1024 + 512 * i, 512), 512)] for i in range(2)]
    qkv = [pieces(wk.at[0], 0, 8, 0), pieces(quarter[0], 1, 4, 8), pieces(quarter[1], 2, 4, 12)]
    kin = _copies([(kc.at[0, i], kb0.at[i]) for i in range(b)], ksem)
    vin = _copies([(vc.at[0, pl.ds(2 * i, 2)], vb0.at[pl.ds(2 * i, 2)]) for i in range(b // 2)], vsem)
    rest = _copies([(wo.at[0], wob), (w1.at[0], w1b), (w2.at[0], w2b)], osem)
    _start(qkv[1] + qkv[2])
    _wait(small)
    grp.enter()

    def arrived(i):
        _wait(qkv[i])
        if i == 1:
            _start(kin)
        if i == 2:
            _start(vin)

    mine = _project(x[...].astype(F32), g1[0:1, :].astype(F32), w, arrived)
    for i in range(3):
        pr[core, i] = mine[i].astype(BF16)
    c = grp.send(pr.at[core], pr.at[core], psem.at[0], psem.at[1], 1)
    c.wait_recv()
    proj = [pr[0, 0], pr[1, 0], pr[0, 1], pr[0, 2], pr[1, 1], pr[1, 2]]
    proj = [t.astype(F32) for t in proj]
    new[0], new[1] = proj[0], proj[1]
    _partials(proj, lens, grp.me * s, kb0, vb0, lambda: _wait(kin), lambda: _wait(vin),
              qs, sn, ps, pn, st, att)
    grp.scatter(att)
    ahead = _qkv_weights(1, wq, wk, wv, wn, nsem) + _copies([(kc.at[1], kb1), (vc.at[1], vb1)], csem)
    for c in rest + ahead:
        c.start()
    grp.layer(x, g2[0:1, :], wob, w1b, w2b, xn, lambda i: rest[i].wait())
    for c in range(2):
        h[:, c * HALF:(c + 1) * HALF] = grp.hb[1, c]
    for c in ahead:
        c.wait()
    grp.leave()


def _second(h, lens, g1, new, kb0_, vb0_, kb1_, vb1_, w,
            att, ko, vo, kb0, vb0, kb1, vb1, qs, sn, ps, pn, st, bsem):
    b, s = kb0.shape[0], kb0.shape[2]
    base = lax.axis_index('sp') * s
    caches = [(kb0, ko, 0), (vb0, vo, 0), (kb1, ko, 1), (vb1, vo, 1)]

    def bulk(n, i):
        src, dst, l = caches[n]
        return pltpu.make_async_copy(src.at[i], dst.at[l, i], bsem.at[n, i])

    def here(i):
        pos = lens[i] - 1 - base
        return (pos >= 0) & (pos < s)

    @pl.loop(0, b)
    def _(i):
        @pl.when(jnp.logical_not(here(i)))
        def _():
            for n in range(4):
                bulk(n, i).start()

    def write(ns, news):
        for i in range(b):
            @pl.when(here(i))
            def _():
                pos = lens[i] - 1 - base
                at = pl.ds(pl.multiple_of(pos // 128 * 128, 128), 128)
                hit = _iota((s, 128), 1) == pos % 128
                for n, x in zip(ns, news):
                    col = jnp.broadcast_to(x[i:i + 1, :], (128, s)).T
                    buf = caches[n][0]
                    buf[i, :, at] = jnp.where(hit, col, buf[i, :, at].astype(F32)).astype(BF16)
                    bulk(n, i).start()

    write((0, 1), (new[0], new[1]))
    proj = _project(h[...], g1[1:2, :].astype(F32), w, lambda i: None)
    write((2, 3), proj[:2])
    _partials(proj, lens, base, kb1, vb1, lambda: None, lambda: None, qs, sn, ps, pn, st, att)
    _wait([bulk(n, i) for n in range(4) for i in range(b)])


def _third(h, att, g2, wo, w1, w2, y, wob, w1b, w2b, xn, osem, *group):
    grp = _Group(group)
    grp.signal()
    rest = _copies([(wo.at[1], wob), (w1.at[1], w1b), (w2.at[1], w2b)], osem)
    for c in rest:
        c.start()
    grp.enter()
    grp.scatter(att)
    grp.layer(h, g2[1:2, :], wob, w1b, w2b, xn, lambda i: rest[i].wait())
    for c in range(2):
        y[:, c * HALF:(c + 1) * HALF] = grp.hb[1, c].astype(y.dtype)
    grp.leave()


def solution(mesh):
    kspec = P(None, 'dp', 'sp', None, None)

    def local(x, lens, wq, wk, wv, wo, w1, w2, g1, g2, kc, vc):
        nl, b, s, kvh, dh = kc.shape
        d = kvh * dh
        kt = kc.transpose(0, 1, 3, 4, 2).reshape(nl, b, d, s)
        vt = vc.transpose(0, 1, 3, 4, 2).reshape(nl, b, d, s)
        slice_, weights = pltpu.VMEM((b, d, s), BF16), pltpu.VMEM((6, wq.shape[1], d), BF16)
        mlp = [pltpu.VMEM(w.shape[1:], BF16) for w in (wo, w1, w2)]
        local_ = [pltpu.VMEM((256, 128), F32), pltpu.VMEM((256, 128), F32), pltpu.VMEM((b, 32, s), BF16),
                  pltpu.VMEM((b, 32, 128), F32), pltpu.VMEM((b, 32, 128), F32)]
        partial = pltpu.VMEM((256, 128), F32)
        rows = pltpu.VMEM(x.shape, BF16)

        def call(body, name, n_in, out_shape, out_specs, scratch, collective_id=None, limit=64, aliases={}):
            return pl.pallas_call(
                body, out_shape=out_shape, in_specs=n_in, out_specs=out_specs, scratch_shapes=scratch,
                input_output_aliases=aliases,
                compiler_params=pltpu.CompilerParams(
                    collective_id=collective_id, has_side_effects=collective_id is not None,
                    vmem_limit_bytes=limit << 20), name=name)

        h, new, *held = call(
            _first, 'first', [HBM] * 12,
            (pltpu.VMEM(x.shape, F32), pltpu.VMEM((2, b, d), F32), slice_, slice_, slice_, slice_, weights),
            (VMEM,) * 7,
            [pltpu.VMEM((3, wq.shape[1], d), BF16), *mlp, *local_, partial, rows,
             DMA((16,)), DMA((6,)), DMA((b,)), DMA((b,)), DMA((3,)), DMA((2,)),
             rows, pltpu.SMEM(lens.shape, lens.dtype), pltpu.VMEM(g1.shape, BF16), pltpu.VMEM(g2.shape, BF16), DMA((4,)),
             pltpu.VMEM((2, 3, b, d), BF16), DMA((2,)),
             *_Group.SCRATCH], 0, limit=22,
        )(*_in(pltpu.HBM, x, lens, g1, g2, wq, wk, wv, wo, w1, w2, kt, vt))
        cache = jax.ShapeDtypeStruct(kt.shape, kt.dtype)
        att, ko, vo, *_ = call(
            _second, 'second', [VMEM, SMEM, VMEM] + [VMEM] * 6,
            (pltpu.VMEM((256, 128), F32), cache, cache) + (slice_,) * 4, (VMEM, HBM, HBM) + (VMEM,) * 4,
            [*local_, DMA((4, b))], limit=8, aliases={4: 3, 5: 4, 6: 5, 7: 6},
        )(h, lens, g1, *_in(pltpu.VMEM, new, *held))
        y = call(
            _third, 'third', [VMEM, VMEM, VMEM] + [HBM] * 3, jax.ShapeDtypeStruct(x.shape, BF16), VMEM,
            [*mlp, rows, DMA((3,)), *_Group.SCRATCH], 1, limit=16,
        )(h, att, g2, *_in(pltpu.HBM, wo, w1, w2))
        back = [t.reshape(nl, b, kvh, dh, s).transpose(0, 1, 4, 2, 3) for t in (ko, vo)]
        return y, *back

    return jax.shard_map(
        local, mesh=mesh,
        in_specs=(P('dp', None), P('dp'), P(), P(), P(), P(None, 'sp', None), P(None, None, 'sp'),
                  P(None, 'sp', None), P(), P(), kspec, kspec),
        out_specs=(P('dp', None), kspec, kspec), check_vma=False)
```
